512 devices in a mesh: row: 16 (over y, x), col: 32 (over z, core).
Axes of the slice: x: 4, y: 4, z: 16, core: 2. Of those that a mesh axis runs over, the one named last changes fastest.
Arguments:
- environment: bfloat16 [768, 16384], P(None, 'row'), may hold values from -6 to 6
- even_site: bfloat16 [16384, 2, 16384], P('row', None, 'col'), may hold values from -0.5 to 0.5
- odd_site: bfloat16 [16384, 2, 16384], P('col', None, 'row'), may hold values from -0.5 to 0.5
- outcomes: int32 [2, 768], replicated, may hold values from 0 to 1
- basis_codes: int32 [2, 768], replicated, may hold values from 0 to 1
Outputs:
- final_environment: bfloat16 [768, 16384], P('col', 'row')
- probabilities: float32 [2, 768], P(None, 'col')
The draws below stay inside these ranges and needn't reach their ends.
Inputs may be any that keep to these rules, and one draw needn't show every extreme that they name: `outcomes`: outcome 0 or 1 of each measurement. `basis_codes`: 0 is the z basis, 1 the x basis.
All inputs are finite; a program needn't handle non-finite values.
Results may differ from the reference program's by a relative error of at most 0.028.
Values may be sent and summed in bfloat16 or wider, within the bound.
A program may use at most 64 MiB of HBM per device.

```python
import jax
import jax.numpy as jnp
from jax import lax

CHI = 16384
SITES = 2
SAMPLES = 768
N_ROW = 16
N_COL = 32


def draw_tensor(key):
    subkeys = jax.random.split(key, 3)
    position = jnp.arange(CHI).astype(jnp.float32) / (CHI - 1) - 0.5
    spin_sign = jnp.array([1.0, -1.0], jnp.float32).reshape(1, 2, 1)
    entries = jnp.clip(jax.random.normal(subkeys[0], (CHI, 2, CHI), jnp.float32), -6.0, 6.0)
    column_scale = jnp.exp(jax.random.uniform(subkeys[1], (CHI,), jnp.float32, 0.0, 2.3026))
    row_scale = jnp.exp(jax.random.uniform(subkeys[2], (CHI, 1, 1), jnp.float32, 0.0, 0.01))
    ramp_rate = 1.0986
    column_scale = column_scale / jnp.sqrt(jnp.mean(column_scale * column_scale))
    row_scale = row_scale / jnp.sqrt(jnp.mean(row_scale * row_scale))
    spin_ramp = jnp.exp(ramp_rate * spin_sign * position.reshape(1, 1, CHI))
    spin_ramp = spin_ramp / jnp.sqrt(jnp.mean(spin_ramp * spin_ramp))
    values = entries * row_scale * column_scale * spin_ramp * CHI ** (-0.5)
    return jnp.clip(values, -0.5, 0.5).astype(jnp.bfloat16)


def draw_even_site(key, part):
    return draw_tensor(jax.random.fold_in(key, 11))


def draw_odd_site(key, part):
    return draw_tensor(jax.random.fold_in(key, 23))


def touch_ends(values, key, smallest, largest):
    index_at = [jax.random.randint(jax.random.fold_in(key, axis), (), 0, length) for axis, length in enumerate(values.shape)]
    main_axis = values.shape.index(max(values.shape))
    next_to = index_at[:main_axis] + [(index_at[main_axis] + 1) % values.shape[main_axis]] + index_at[main_axis + 1:]
    return values.at[tuple(index_at)].set(smallest).at[tuple(next_to)].set(largest)


def level_of(key, dims, cuts, smallest, top_value):
    def one(dim, shards_of):
        heights = jax.random.uniform(jax.random.fold_in(jax.random.fold_in(key, 6), dim), (shards_of,), jnp.float32, smallest / len(cuts), top_value / len(cuts))
        return jnp.repeat(jnp.exp(heights), dims[dim] // shards_of).reshape((-1,) + (1,) * (len(dims) - dim - 1))

    loudness = one(*cuts[0])
    for cut in cuts[1:]:
        loudness = loudness * one(*cut)
    return loudness


def scatter_about(own_key, shape, deviation, reach, cuts=(), held_as=jnp.bfloat16):
    gain = level_of(own_key, shape, cuts, -0.22, 0.18) if cuts else 1.0
    values = jax.random.normal(own_key, shape, jnp.float32) * deviation * gain
    return jnp.minimum(jnp.maximum(values, -reach), reach).astype(held_as)


def setup_inputs(seed: int = 0) -> dict:
    streams_of = jax.random.split(jax.random.key(seed), 6)
    environment = scatter_about(streams_of[0], (SAMPLES, CHI), 1.0, 6.0, ((1, 16),))
    even_site = draw_even_site(jax.random.fold_in(streams_of[5], 71), 0)
    odd_site = draw_odd_site(jax.random.fold_in(streams_of[5], 71), 0)
    outcomes = touch_ends(jax.random.randint(streams_of[3], (SITES, SAMPLES), 0, 2), jax.random.fold_in(streams_of[3], 1), 0, 1).astype(jnp.int32)
    basis_codes = touch_ends(jax.random.randint(streams_of[4], (SITES, SAMPLES), 0, 2), jax.random.fold_in(streams_of[4], 1), 0, 1).astype(jnp.int32)
    return dict(environment=environment, even_site=even_site, odd_site=odd_site, outcomes=outcomes, basis_codes=basis_codes)


half_root = 0.7071067811865476

def site_sum(vectors, tensor, blocks):
    span = CHI // blocks
    tensor_rows = tensor.reshape(blocks, span, 2 * CHI)
    vector_cols = vectors.reshape(SAMPLES, blocks, span).transpose(1, 0, 2)

    def add_block(carry, pieces):
        term = jnp.dot(pieces[0], pieces[1], preferred_element_type=jnp.float32)
        rounded = lax.optimization_barrier(term.astype(jnp.bfloat16))
        return (carry + rounded.astype(jnp.float32), None)
    start_sum = jnp.zeros((SAMPLES, 2 * CHI), jnp.float32)
    summed, unused = lax.scan(add_block, start_sum, (vector_cols, tensor_rows))
    return summed.reshape(SAMPLES, 2, CHI)

def collapse(summed, basis_row, outcome_row):
    upper = summed[:, 0, :]
    lower = summed[:, 1, :]
    rotate = (basis_row == 1)[:, None]
    first = jnp.where(rotate, (upper + lower) * half_root, upper)
    second = jnp.where(rotate, (upper - lower) * half_root, lower)
    norm_first = lax.optimization_barrier(jnp.sum(first * first, axis=1))
    norm_second = lax.optimization_barrier(jnp.sum(second * second, axis=1))
    pick = outcome_row == 1
    chosen = jnp.where(pick[:, None], second, first)
    chosen_norm = jnp.where(pick, norm_second, norm_first)
    return (chosen, chosen_norm, chosen_norm / (norm_first + norm_second))

def reference(environment, even_site, odd_site, outcomes, basis_codes):
    summed = site_sum(environment, even_site, N_ROW)
    chosen, chosen_norm, prob_first = collapse(summed, basis_codes[0], outcomes[0])
    projected = chosen.astype(jnp.bfloat16)
    summed = site_sum(projected, odd_site, N_COL)
    chosen, chosen_norm, prob_second = collapse(summed, basis_codes[1], outcomes[1])
    final_environment = (chosen * jnp.sqrt(CHI / chosen_norm)[:, None]).astype(jnp.bfloat16)
    probabilities = jnp.stack([prob_first, prob_second], axis=0)
    return (final_environment, probabilities)
```

```python
import jax
import jax.numpy as jnp
from jax import lax
from jax.experimental import pallas as pl
from jax.experimental.pallas import tpu as pltpu
from jax.sharding import PartitionSpec as P

CHI = 16384
HALF_ROOT = 0.7071067811865476
F32 = jnp.float32
BF16 = jnp.bfloat16
MESH = pl.DeviceIdType.MESH

NA = 4
NZ = 16
G = NA * NA
HZ = NZ // 2
GROUP = 24
NB = 3
SB = GROUP // NB
R = 2 * SB
COLS = 512
RIGHT = 1024


def coefficients(sel):
    rotated = sel >= 1.5
    odd = (sel == 1.0) | (sel == 3.0)
    sign = jnp.where(odd, -HALF_ROOT, HALF_ROOT)
    a = jnp.where(rotated, HALF_ROOT, jnp.where(odd, 0.0, 1.0))
    b = jnp.where(rotated, sign, jnp.where(odd, 1.0, 0.0))
    c = jnp.where(rotated, HALF_ROOT, jnp.where(odd, 1.0, 0.0))
    d = jnp.where(rotated, -sign, jnp.where(odd, 0.0, 1.0))
    return ((a, b), (c, d))


def kernel(
    env_hbm,
    te_hbm,
    to_hbm,
    outcomes,
    basis,
    out_ref,
    prob_ref,
    env_v,
    te_v,
    to_v,
    flat,
    w0,
    acc0,
    sel,
    s1,
    r1,
    s2,
    r2,
    g_buf,
    lhs,
    tb,
    acc1,
    part,
    zs,
    zr,
    fin,
    msg,
    n0r,
    nfs,
    nfr,
    load_sem,
    s1_sem,
    r1_sem,
    s2_sem,
    r2_sem,
    ga_ssem,
    ga_rsem,
    gb_ssem,
    gb_rsem,
    tb_ssem,
    tb_rsem,
    z_ssem,
    z_rsem,
    n0_ssem,
    n0_rsem,
    nf_ssem,
    nf_rsem,
):
    row = lax.axis_index("row")
    col = lax.axis_index("col")
    z = col // 2
    core = col % 2
    x = row % NA
    y = row // NA
    first_place = (x, y)
    second_place = (y, x)

    def at(px, py, pz, pc):
        return {"row": py * NA + px, "col": pz * 2 + pc}

    def peer(f, a, b, pc):
        return at(a, b, z, pc) if f == 0 else at(b, a, z, pc)

    def send(src, dst, ssem, rsem, device):
        pltpu.make_async_remote_copy(
            src_ref=src, dst_ref=dst, send_sem=ssem, recv_sem=rsem, device_id=device, device_id_type=MESH
        ).start()

    def wait_bytes(ref, sem):
        pltpu.make_async_copy(ref, ref, sem).wait()

    loads = [
        pltpu.make_async_copy(te_hbm, te_v, load_sem.at[0]),
        pltpu.make_async_copy(env_hbm, env_v, load_sem.at[1]),
        pltpu.make_async_copy(to_hbm, to_v, load_sem.at[2]),
    ]
    for load in loads:
        load.start()

    barrier = pltpu.get_barrier_semaphore()

    def hello(device):
        pl.semaphore_signal(barrier, inc=1, device_id=device, device_id_type=MESH)

    for dx in range(NA):
        for dy in range(NA):
            for dc in range(2):
                if dx == 0 and dy == 0 and dc == 0:
                    continue
                if dc == 1 and dx != 0 and dy != 0:
                    continue
                hello(at((x + dx) % NA, (y + dy) % NA, z, (core + dc) % 2))
    for dz in range(1, NZ):
        hello(at(x, y, (z + dz) % NZ, core))

    eye = lax.broadcasted_iota(jnp.int32, (128, 128), 0) == lax.broadcasted_iota(jnp.int32, (128, 128), 1)
    for s in range(2):
        for j in range(6):
            lanes = slice(j * 128, (j + 1) * 128)
            code = (2 * basis[s : s + 1, lanes] + outcomes[s : s + 1, lanes]).astype(F32)
            column = jnp.sum(jnp.where(eye, jnp.broadcast_to(code, (128, 128)), 0.0), axis=1, keepdims=True)
            sel[s, j * 128 : (j + 1) * 128, :] = jnp.broadcast_to(column, (128, 128))

    loads[0].wait()

    def spread_even(i, carry):
        l0 = pl.multiple_of(i * 128, 128)
        flat[0:1024, :] = te_v[pl.ds(l0, 128)].astype(F32).reshape(1024, 128)
        for lt in range(4):
            for s in range(2):
                w0[pl.ds(l0, 128), s * COLS + lt * 128 : s * COLS + lt * 128 + 128] = flat[
                    pl.ds(lt * 2 + s, 128, stride=8), :
                ].astype(BF16)
        return carry

    lax.fori_loop(0, 8, spread_even, 0)
    loads[1].wait()

    def multiply_first(i, carry):
        m0 = pl.multiple_of(i * 256, 256)
        rows = env_v[pl.ds(i * 32, 32)].reshape(256, 1024)
        for n in range(2):
            acc0[pl.ds(m0, 256), n * 512 : n * 512 + 512] = jnp.dot(
                rows, w0[:, n * 512 : n * 512 + 512], preferred_element_type=F32
            )
        return carry

    lax.fori_loop(0, 3, multiply_first, 0)

    def build_first(k, v):
        def one(gp, carry):
            g = gp // 2
            p = gp % 2
            gx = g % NA
            gy = g // NA
            rows = pl.ds(pl.multiple_of(gp * GROUP + k * SB, 8), SB)
            cu, cd = coefficients(sel[0, rows, :])[v]
            for f in range(2):
                halves = []
                for h in range(2):
                    lo = h * 256 + f * 128
                    halves.append(cu * acc0[rows, lo : lo + 128] + cd * acc0[rows, COLS + lo : COLS + lo + 128])
                ga, gb = (gx, gy) if f == 0 else (gy, gx)
                s1[k, v, f, p, ga, gb] = jnp.concatenate(halves, axis=0).astype(BF16)
            return carry

        lax.fori_loop(0, 2 * G, one, 0)

    def send_first(k, v):
        for da in (2, 1, 3, 0):
            for f in range(2):
                a = (first_place[f] + da) % NA
                for dc in range(2):
                    if da == 0 and dc == 0:
                        continue
                    pc = (core + dc) % 2
                    send(
                        s1.at[k, v, f, pc, a],
                        r1.at[k, v, f, first_place[f] * 2 + core],
                        s1_sem,
                        r1_sem.at[k, v, f],
                        peer(f, a, second_place[f], pc),
                    )

    def reduce_first(k, v):
        for f in range(2):
            r1[k, v, f, first_place[f] * 2 + core] = s1[k, v, f, core, first_place[f]]
            wait_bytes(r1.at[k, v, f, 0:7], r1_sem.at[k, v, f])
            for b in range(NA):
                for c in range(2):
                    total = r1[k, v, f, c, b].astype(F32)
                    for a in range(1, NA):
                        total = total + r1[k, v, f, a * 2 + c, b].astype(F32)
                    s2[k, v, f, b, c] = total.astype(BF16)
            for db in (2, 1, 3):
                b = (second_place[f] + db) % NA
                send(
                    s2.at[k, v, f, b],
                    r2.at[k, v, f, second_place[f]],
                    s2_sem,
                    r2_sem.at[k, v, f],
                    peer(f, first_place[f], b, core),
                )

    lane = lax.broadcasted_iota(jnp.int32, (SB, 128), 1)
    sub = lax.broadcasted_iota(jnp.int32, (SB, 128), 0)

    def norms_to_lanes(squares, base):
        sums = jnp.sum(squares, axis=1, keepdims=True)
        column = sums[:SB] + sums[SB:]
        return jnp.sum(jnp.where(lane == sub + base, column, 0.0), axis=0, keepdims=True)

    def finish_first(k, v):
        squares = jnp.zeros((R, 128), F32)
        for f in range(2):
            r2[k, v, f, second_place[f]] = s2[k, v, f, second_place[f]]
            wait_bytes(r2.at[k, v, f, 0:3], r2_sem.at[k, v, f])
            for c in range(2):
                total = r2[k, v, f, 0, c].astype(F32)
                for b in range(1, NA):
                    total = total + r2[k, v, f, b, c].astype(F32)
                squares = squares + total * total
                if v == 0:
                    g_buf[k, f, first_place[f], second_place[f], c] = total.astype(BF16)
            if v == 0:
                for db in (2, 1, 3):
                    b = (second_place[f] + db) % NA
                    here = g_buf.at[k, f, first_place[f], second_place[f]]
                    send(here, here, ga_ssem, ga_rsem.at[k, f], peer(f, first_place[f], b, core))
        msg[0:1, :] += norms_to_lanes(squares, 64 + 32 * v + k * SB)

    def pass_on(k):
        for f in range(2):
            wait_bytes(g_buf.at[k, f, 0, 0:3], ga_rsem.at[k, f])
            for da in (2, 1, 3):
                a = (first_place[f] + da) % NA
                here = g_buf.at[k, f, first_place[f]]
                send(here, here, gb_ssem, gb_rsem.at[k, f], peer(f, a, second_place[f], core))

    def multiply_second(k):
        for f in range(2):
            wait_bytes(g_buf.at[k, f, 0:3], gb_rsem.at[k, f])

        def pair(j, carry):
            m0 = pl.multiple_of(j * 2 * SB, 2 * SB)
            gy = j // 2
            for f in range(2):
                for c in range(2):
                    two = []
                    for e in range(2):
                        gx = (2 * j + e) % NA
                        ga, gb = (gx, gy) if f == 0 else (gy, gx)
                        two.append(g_buf[k, f, ga, gb, c].astype(F32))
                    for h in range(2):
                        lo = h * 512 + c * 256 + f * 128
                        lhs[pl.ds(m0, 2 * SB), lo : lo + 128] = jnp.concatenate(
                            [t[h * SB : (h + 1) * SB] for t in two], axis=0
                        ).astype(BF16)
            return carry

        lax.fori_loop(0, G // 2, pair, 0)
        left = lhs[...]

        def columns(n, carry):
            cols = pl.ds(pl.multiple_of(n * 256, 256), 256)
            acc1[:, cols] = jnp.dot(left, tb[:, :, :, cols].reshape(1024, 256), preferred_element_type=F32)
            return carry

        lax.fori_loop(0, 8, columns, 0)

        def one(g, carry):
            rows = pl.ds(pl.multiple_of(g * SB, 8), SB)
            samples = pl.ds(pl.multiple_of((2 * g + core) * GROUP + k * SB, 8), SB)
            pairs = coefficients(sel[1, samples, :])
            for v in range(2):
                cu, cd = pairs[v]
                for t in range(4):
                    halves = []
                    for h in range(2):
                        lo = h * 512 + t * 128
                        halves.append(
                            cu * acc1[rows, lo : lo + 128] + cd * acc1[rows, RIGHT + lo : RIGHT + lo + 128]
                        )
                    part[k, v, g, :, t * 128 : t * 128 + 128] = jnp.concatenate(halves, axis=0).astype(BF16)
            return carry

        lax.fori_loop(0, G, one, 0)

    def hops(v, d):
        return HZ - v if d == 0 else HZ - 1 + v

    def slot(v, d, s):
        return {(0, 0): 0, (0, 1): HZ, (1, 0): 2 * HZ - 1, (1, 1): 3 * HZ - 2}[v, d] + s

    def ring_step(k, s):
        for v in range(2):
            for d in range(2):
                n = hops(v, d)
                if s >= n:
                    continue
                owner = (z + n - s) % NZ if d == 0 else (z + NZ - n + s) % NZ
                step = 1 if d == 0 else NZ - 1
                here = slot(v, d, s)
                if s == 0:
                    src = part.at[k, v, owner]
                else:
                    wait_bytes(zr.at[k, here - 1], z_rsem.at[k, here - 1])
                    zs[k, here] = (zr[k, here - 1].astype(F32) + part[k, v, owner].astype(F32)).astype(BF16)
                    src = zs.at[k, here]
                send(src, zr.at[k, here], z_ssem, z_rsem.at[k, here], at(x, y, (z + step) % NZ, core))

    def ring_end(k):
        for v in range(2):
            total = part[k, v, z].astype(F32)
            for d in range(2):
                last = slot(v, d, hops(v, d) - 1)
                wait_bytes(zr.at[k, last], z_rsem.at[k, last])
                total = total + zr[k, last].astype(F32)
            if v == 0:
                fin[k * SB : (k + 1) * SB, 0:512] = total[:SB]
                fin[k * SB : (k + 1) * SB, 512:1024] = total[SB:]
            msg[1:2, :] += norms_to_lanes(total * total, 32 * v + k * SB)

    msg[...] = jnp.zeros_like(msg)
    pl.semaphore_wait(barrier, 37)

    for k in range(NB):
        build_first(k, 0)
        send_first(k, 0)

    loads[2].wait()

    def spread_odd(i, carry):
        flat[...] = to_v[pl.ds(i * 256, 256)].astype(F32).reshape(2048, 128)
        h = i // 2
        w = pl.multiple_of((i % 2) * 128, 128)
        for lt in range(8):
            for s in range(2):
                lo = s * RIGHT + lt * 128
                tb[h, core, pl.ds(w, 128), lo : lo + 128] = flat[pl.ds(lt * 2 + s, 128, stride=16), :].astype(BF16)
        return carry

    lax.fori_loop(0, 4, spread_odd, 0)
    for h in range(2):
        send(tb.at[h, core], tb.at[h, core], tb_ssem, tb_rsem, at(x, y, z, 1 - core))
    for k in range(NB):
        build_first(k, 1)

    for k in range(NB):
        reduce_first(k, 0)
    for k in range(NB):
        finish_first(k, 0)
    for k in range(NB):
        pass_on(k)
    for k in range(NB):
        send_first(k, 1)
    wait_bytes(tb.at[:, 0], tb_rsem)

    for tick in range(HZ + NB):
        if tick < NB:
            multiply_second(tick)
        for k in range(NB - 1, -1, -1):
            s = tick - k
            if 0 <= s < HZ:
                ring_step(k, s)
            elif s == HZ:
                ring_end(k)
        if tick == NB:
            for k in range(NB):
                reduce_first(k, 1)
        if tick == NB + 2:
            for k in range(NB):
                finish_first(k, 1)
            n0r[z] = msg[0:1, :]
            nfs[0:1, :] = msg[0:1, :]

            @pl.when(z != row)
            def _():
                send(nfs.at[0:1], n0r.at[z], n0_ssem, n0_rsem, at(x, y, row, core))

    nfs[1:2, :] = msg[1:2, :]

    @pl.when(z == row)
    def _():
        wait_bytes(n0r.at[0 : NZ - 1], n0_rsem)
        nfs[1:2, :] = msg[1:2, :] + jnp.sum(n0r[...], axis=0)

    nfr[row] = nfs[1:2, :]
    for dx in range(NA):
        for dy in range(NA):
            if dx or dy:
                send(nfs.at[1:2], nfr.at[row], nf_ssem, nf_rsem, at((x + dx) % NA, (y + dy) % NA, z, core))
    wait_bytes(nfr.at[0 : G - 1], nf_rsem)
    norms = jnp.sum(nfr[...], axis=0)
    prob = norms / (norms + pltpu.roll(norms, 96, 1))
    prob_ref[0:1, :] = pltpu.roll(prob, 64, 1)[:, :GROUP]
    prob_ref[1:2, :] = prob[:, :GROUP]
    lane24 = lax.broadcasted_iota(jnp.int32, (GROUP, 128), 1)
    sub24 = lax.broadcasted_iota(jnp.int32, (GROUP, 128), 0)
    column = jnp.sum(jnp.where(lane24 == sub24, jnp.broadcast_to(norms, (GROUP, 128)), 0.0), axis=1, keepdims=True)
    out_ref[...] = (fin[...] * jnp.sqrt(CHI / column)).astype(BF16)

    wait_bytes(r1.at[:, :, :, 0:7], s1_sem)
    wait_bytes(r2.at[:, :, :, 0:3], s2_sem)
    wait_bytes(g_buf.at[:, :, 0, 0:3], ga_ssem)
    wait_bytes(g_buf.at[:, :, 0:3], gb_ssem)
    wait_bytes(tb.at[:, 0], tb_ssem)
    wait_bytes(zr, z_ssem)

    @pl.when(z != row)
    def _():
        wait_bytes(n0r.at[0], n0_ssem)

    wait_bytes(nfr.at[0 : G - 1], nf_ssem)


def per_device(environment, even_site, odd_site, outcomes, basis_codes):
    samples, left = environment.shape
    env = environment.reshape(samples // 8, 8, left)
    te = even_site.reshape(left, 2, 4, 128).transpose(0, 2, 1, 3).reshape(left, 8, 128)
    to = odd_site.reshape(512, 2, 8, 128).transpose(0, 2, 1, 3).reshape(1024, 8, 128)
    vmem = pl.BlockSpec(memory_space=pltpu.VMEM)
    hbm = pl.BlockSpec(memory_space=pl.ANY)
    dma = pltpu.SemaphoreType.DMA
    nz_slots = 4 * HZ - 2
    return pl.pallas_call(
        kernel,
        out_shape=(
            jax.ShapeDtypeStruct((GROUP, RIGHT), BF16),
            jax.ShapeDtypeStruct((2, GROUP), F32),
        ),
        in_specs=[hbm, hbm, hbm, vmem, vmem],
        out_specs=(vmem, vmem),
        scratch_shapes=[
            pltpu.VMEM((samples // 8, 8, left), BF16),
            pltpu.VMEM((left, 8, 128), BF16),
            pltpu.VMEM((1024, 8, 128), BF16),
            pltpu.VMEM((2048, 128), F32),
            pltpu.VMEM((left, 2 * COLS), BF16),
            pltpu.VMEM((samples, 2 * COLS), F32),
            pltpu.VMEM((2, samples, 128), F32),
            pltpu.VMEM((NB, 2, 2, 2, NA, NA, R, 128), BF16),
            pltpu.VMEM((NB, 2, 2, 2 * NA, NA, R, 128), BF16),
            pltpu.VMEM((NB, 2, 2, NA, 2, R, 128), BF16),
            pltpu.VMEM((NB, 2, 2, NA, 2, R, 128), BF16),
            pltpu.VMEM((NB, 2, NA, NA, 2, R, 128), BF16),
            pltpu.VMEM((G * SB, 1024), BF16),
            pltpu.VMEM((2, 2, 256, 2 * RIGHT), BF16),
            pltpu.VMEM((G * SB, 2 * RIGHT), F32),
            pltpu.VMEM((NB, 2, NZ, R, 512), BF16),
            pltpu.VMEM((NB, nz_slots, R, 512), BF16),
            pltpu.VMEM((NB, nz_slots, R, 512), BF16),
            pltpu.VMEM((GROUP, RIGHT), F32),
            pltpu.VMEM((8, 128), F32),
            pltpu.VMEM((NZ, 1, 128), F32),
            pltpu.VMEM((8, 128), F32),
            pltpu.VMEM((G, 1, 128), F32),
            dma((3,)),
            dma,
            dma((NB, 2, 2)),
            dma,
            dma((NB, 2, 2)),
            dma,
            dma((NB, 2)),
            dma,
            dma((NB, 2)),
            dma,
            dma,
            dma,
            dma((NB, nz_slots)),
            dma,
            dma,
            dma,
            dma,
        ],
        compiler_params=pltpu.CompilerParams(
            collective_id=0, has_side_effects=True, vmem_limit_bytes=60 * 1024 * 1024
        ),
    )(env, te, to, outcomes, basis_codes)


def solution(mesh):
    placed = (P(None, "row"), P("row", None, "col"), P("col", None, "row"), P(), P())
    return jax.shard_map(
        per_device,
        mesh=mesh,
        in_specs=placed,
        out_specs=(P("col", "row"), P(None, "col")),
        check_vma=False,
    )
```

```python
import jax
import jax.numpy as jnp
from jax import lax
from jax.experimental import pallas as pl
from jax.experimental.pallas import tpu as pltpu
from jax.sharding import PartitionSpec as P

CHI = 16384
HALF_ROOT = 0.7071067811865476
F32 = jnp.float32
BF16 = jnp.bfloat16
MESH = pl.DeviceIdType.MESH

NA = 4
NZ = 16
G = NA * NA
HZ = NZ // 2
GROUP = 24
NB = 3
SB = GROUP // NB
R = 2 * SB
COLS = 512
RIGHT = 1024
NQ = 4
LW = 512 // NQ
RZ = 2 * GROUP


def coefficients(sel):
    rotated = sel >= 1.5
    odd = (sel == 1.0) | (sel == 3.0)
    sign = jnp.where(odd, -HALF_ROOT, HALF_ROOT)
    a = jnp.where(rotated, HALF_ROOT, jnp.where(odd, 0.0, 1.0))
    b = jnp.where(rotated, sign, jnp.where(odd, 1.0, 0.0))
    c = jnp.where(rotated, HALF_ROOT, jnp.where(odd, 1.0, 0.0))
    d = jnp.where(rotated, -sign, jnp.where(odd, 0.0, 1.0))
    return ((a, b), (c, d))


def kernel(
    env_hbm,
    te_hbm,
    to_hbm,
    outcomes_hbm,
    basis_hbm,
    out_ref,
    chosen_ref,
    both_ref,
    env_v,
    te_v,
    to_v,
    outcomes,
    basis,
    flat,
    w0,
    acc0,
    sel,
    s1,
    r1,
    s2,
    r2,
    r2o,
    g_buf,
    lhs,
    tb,
    acc1,
    part,
    zs,
    zr,
    fin,
    square,
    msg,
    n0r,
    nfs,
    nfr,
    load_sem,
    te_sem,
    s1_sem,
    r1_sem,
    s2_sem,
    s2o_sem,
    r2_sem,
    gb_ssem,
    gb_rsem,
    tb_ssem,
    tb_rsem,
    z_ssem,
    z_rsem,
    n0_ssem,
    n0_rsem,
    nf_ssem,
    nf_rsem,
    known,
):
    row = lax.axis_index("row")
    col = lax.axis_index("col")
    z = col // 2
    core = col % 2
    x = row % NA
    y = row // NA
    first_place = (x, y)
    second_place = (y, x)

    def at(px, py, pz, pc):
        return {"row": py * NA + px, "col": pz * 2 + pc}

    def peer(f, a, b, pc):
        return at(a, b, z, pc) if f == 0 else at(b, a, z, pc)

    def send(src, dst, ssem, rsem, device):
        pltpu.make_async_remote_copy(
            src_ref=src, dst_ref=dst, send_sem=ssem, recv_sem=rsem, device_id=device, device_id_type=MESH
        ).start()

    def wait_bytes(ref, sem):
        pltpu.make_async_copy(ref, ref, sem).wait()

    codes = [
        pltpu.make_async_copy(outcomes_hbm, outcomes, load_sem.at[0]),
        pltpu.make_async_copy(basis_hbm, basis, load_sem.at[1]),
    ]
    even = [
        pltpu.make_async_copy(te_hbm.at[pl.ds(i * 256, 256)], te_v.at[pl.ds(i * 256, 256)], te_sem.at[i])
        for i in range(4)
    ]
    vectors = pltpu.make_async_copy(env_hbm, env_v, load_sem.at[2])
    odd = pltpu.make_async_copy(to_hbm, to_v, load_sem.at[3])
    for load in (*even, *codes, vectors):
        load.start()

    barrier = pltpu.get_barrier_semaphore()

    def signal(sem, device):
        pl.semaphore_signal(sem, inc=1, device_id=device, device_id_type=MESH)

    for dc in range(2):
        if dc:
            signal(barrier, at(x, y, z, 1 - core))
        for d in range(1, NA):
            signal(barrier, at((x + d) % NA, y, z, (core + dc) % 2))
            signal(barrier, at(x, (y + d) % NA, z, (core + dc) % 2))
    for dz in (1, NZ - 1):
        signal(barrier, at(x, y, (z + dz) % NZ, core))

    def tell(i):
        for dz in (2**i, NZ - 2**i):
            signal(known.at[i], at(x, y, (z + dz) % NZ, core))

    def hear(i):
        pl.semaphore_wait(known.at[i], 2)

    for i in range(4):
        even[i].wait()
        for j in range(2):
            l0 = i * 256 + j * 128
            flat[j * 1024 : j * 1024 + 1024, :] = te_v[l0 : l0 + 128].astype(F32).reshape(1024, 128)
            for lt in range(4):
                for s in range(2):
                    lo = s * COLS + lt * 128
                    w0[l0 : l0 + 128, lo : lo + 128] = flat[
                        pl.ds(j * 1024 + lt * 2 + s, 128, stride=8), :
                    ].astype(BF16)
    odd.start()

    for load in codes:
        load.wait()
    eye = lax.broadcasted_iota(jnp.int32, (128, 128), 0) == lax.broadcasted_iota(jnp.int32, (128, 128), 1)
    for s in range(2):
        for j in range(6):
            lanes = slice(j * 128, (j + 1) * 128)
            code = (2 * basis[s : s + 1, lanes] + outcomes[s : s + 1, lanes]).astype(F32)
            column = jnp.sum(jnp.where(eye, jnp.broadcast_to(code, (128, 128)), 0.0), axis=1, keepdims=True)
            sel[s, j * 128 : (j + 1) * 128, :] = jnp.broadcast_to(column, (128, 128))
    vectors.wait()

    def multiply_first(k):
        rows = env_v[:, k].reshape(2 * G * SB, 1024)
        for n in range(2):
            acc0[k, :, n * 512 : n * 512 + 512] = jnp.dot(
                rows, w0[:, n * 512 : n * 512 + 512], preferred_element_type=F32
            )

    def build_first(k, v):
        def one(gp, carry):
            g = gp // 2
            p = gp % 2
            gx = g % NA
            gy = g // NA
            rows = pl.ds(pl.multiple_of(gp * SB, 8), SB)
            cu, cd = coefficients(sel[0, pl.ds(pl.multiple_of(gp * GROUP + k * SB, 8), SB), :])[v]
            for f in range(2):
                halves = []
                for h in range(2):
                    lo = h * 256 + f * 128
                    halves.append(
                        cu * acc0[k, rows, lo : lo + 128] + cd * acc0[k, rows, COLS + lo : COLS + lo + 128]
                    )
                ga, gb = (gx, gy) if f == 0 else (gy, gx)
                s1[k, v, f, p, ga, gb] = jnp.concatenate(halves, axis=0).astype(BF16)
            return carry

        lax.fori_loop(0, 2 * G, one, 0, unroll=4)

    def send_first(k, v):
        for da in (2, 1, 3, 0):
            for f in range(2):
                a = (first_place[f] + da) % NA
                for dc in range(2):
                    if da == 0 and dc == 0:
                        continue
                    pc = (core + dc) % 2
                    send(
                        s1.at[k, v, f, pc, a],
                        r1.at[k, v, f, first_place[f] * 2 + core],
                        s1_sem,
                        r1_sem.at[k, v, f],
                        peer(f, a, second_place[f], pc),
                    )

    def reduce_first(k, v):
        for f in range(2):
            r1[k, v, f, first_place[f] * 2 + core] = s1[k, v, f, core, first_place[f]]
            wait_bytes(r1.at[k, v, f, 0:7], r1_sem.at[k, v, f])
            for b in range(NA):
                for c in range(2):
                    total = r1[k, v, f, c, b].astype(F32)
                    for a in range(1, NA):
                        total = total + r1[k, v, f, a * 2 + c, b].astype(F32)
                    s2[k, v, f, b, c] = total.astype(BF16)
            for db in (2, 1, 3):
                b = (second_place[f] + db) % NA
                device = peer(f, first_place[f], b, core)
                if v == 0:
                    send(s2.at[k, v, f], r2.at[k, f, second_place[f]], s2_sem, r2_sem.at[k, v, f], device)
                else:
                    send(s2.at[k, v, f, b], r2o.at[k, f, second_place[f]], s2o_sem, r2_sem.at[k, v, f], device)

    lane = lax.broadcasted_iota(jnp.int32, (GROUP, 128), 1)
    sub = lax.broadcasted_iota(jnp.int32, (GROUP, 128), 0)

    def norms_to_lanes(squares, count, base):
        sums = jnp.sum(squares, axis=1, keepdims=True)
        column = sums[:count] + sums[count:]
        return jnp.sum(jnp.where(lane[:count] == sub[:count] + base, column, 0.0), axis=0, keepdims=True)

    def finish_chosen(k):
        squares = jnp.zeros((R, 128), F32)
        for f in range(2):
            r2[k, f, second_place[f]] = s2[k, 0, f]
            wait_bytes(r2.at[k, f, 0:3], r2_sem.at[k, 0, f])
            for b in range(NA):
                for c in range(2):
                    total = r2[k, f, 0, b, c].astype(F32)
                    for e in range(1, NA):
                        total = total + r2[k, f, e, b, c].astype(F32)
                    g_buf[k, f, first_place[f], b, c] = total.astype(BF16)
            for da in (2, 1, 3):
                a = (first_place[f] + da) % NA
                here = g_buf.at[k, f, first_place[f]]
                send(here, here, gb_ssem, gb_rsem.at[k, f], peer(f, a, second_place[f], core))
        for f in range(2):
            for c in range(2):
                total = r2[k, f, 0, second_place[f], c].astype(F32)
                for e in range(1, NA):
                    total = total + r2[k, f, e, second_place[f], c].astype(F32)
                squares = squares + total * total
        msg[0:1, :] += norms_to_lanes(squares, SB, 64 + k * SB)

    def finish_other(k):
        squares = jnp.zeros((R, 128), F32)
        for f in range(2):
            r2o[k, f, second_place[f]] = s2[k, 1, f, second_place[f]]
            wait_bytes(r2o.at[k, f, 0:3], r2_sem.at[k, 1, f])
            for c in range(2):
                total = r2o[k, f, 0, c].astype(F32)
                for e in range(1, NA):
                    total = total + r2o[k, f, e, c].astype(F32)
                squares = squares + total * total
        msg[0:1, :] += norms_to_lanes(squares, SB, 96 + k * SB)

    def gather_left(k):
        for f in range(2):
            wait_bytes(g_buf.at[k, f, 0:3], gb_rsem.at[k, f])

        def pair(j, carry):
            m0 = pl.multiple_of(k * G * SB + j * 2 * SB, 2 * SB)
            gy = j // 2
            for f in range(2):
                for c in range(2):
                    two = []
                    for e in range(2):
                        gx = (2 * j + e) % NA
                        ga, gb = (gx, gy) if f == 0 else (gy, gx)
                        two.append(g_buf[k, f, ga, gb, c].astype(F32))
                    for h in range(2):
                        lo = h * 512 + c * 256 + f * 128
                        lhs[pl.ds(m0, 2 * SB), lo : lo + 128] = jnp.concatenate(
                            [t[h * SB : (h + 1) * SB] for t in two], axis=0
                        ).astype(BF16)
            return carry

        lax.fori_loop(0, G // 2, pair, 0, unroll=2)

    def multiply_second(q):
        for n in range(4 * LW // 256):
            lo = q * 4 * LW + n * 256
            acc1[q, :, n * 256 : n * 256 + 256] = jnp.dot(
                lhs[...], tb[:, :, :, lo : lo + 256].reshape(1024, 256), preferred_element_type=F32
            )

        def one(g, carry):
            pairs = []
            for k in range(NB):
                samples = pl.ds(pl.multiple_of((2 * g + core) * GROUP + k * SB, 8), SB)
                pairs.append(coefficients(sel[1, samples, :]))
            for t in range(LW // 128):
                chunks = ([], [])
                for h in range(2):
                    for k in range(NB):
                        rows = pl.ds(pl.multiple_of(k * G * SB + g * SB, 8), SB)
                        lo = h * LW + t * 128
                        up = acc1[q, rows, lo : lo + 128]
                        down = acc1[q, rows, 2 * LW + lo : 2 * LW + lo + 128]
                        for v in range(2):
                            cu, cd = pairs[k][v]
                            chunks[v].append(cu * up + cd * down)
                for v in range(2):
                    part[v, q, g, :, t * 128 : t * 128 + 128] = jnp.concatenate(chunks[v], axis=0).astype(BF16)
            return carry

        lax.fori_loop(0, G, one, 0, unroll=2)

    def hops(v, d):
        return HZ - v if d == 0 else HZ - 1 + v

    def slot(v, d, s):
        return {(0, 0): 0, (0, 1): HZ, (1, 0): 2 * HZ - 1, (1, 1): 3 * HZ - 2}[v, d] + s

    def ring_step(q, s):
        for v in range(2):
            for d in range(2):
                n = hops(v, d)
                if s >= n:
                    continue
                owner = (z + n - s) % NZ if d == 0 else (z + NZ - n + s) % NZ
                step = 1 if d == 0 else NZ - 1
                here = slot(v, d, s)
                if s == 0:
                    src = part.at[v, q, owner]
                else:
                    wait_bytes(zr.at[q, here - 1], z_rsem.at[q, here - 1])
                    zs[q, here] = (zr[q, here - 1].astype(F32) + part[v, q, owner].astype(F32)).astype(BF16)
                    src = zs.at[q, here]
                send(src, zr.at[q, here], z_ssem, z_rsem.at[q, here], at(x, y, (z + step) % NZ, core))

    def ring_end(q):
        for v in range(2):
            total = part[v, q, z].astype(F32)
            for d in range(2):
                last = slot(v, d, hops(v, d) - 1)
                wait_bytes(zr.at[q, last], z_rsem.at[q, last])
                total = total + zr[q, last].astype(F32)
            if v == 0:
                for h in range(2):
                    fin[:, h * 512 + q * LW : h * 512 + q * LW + LW] = total[h * GROUP : (h + 1) * GROUP]
            squares = total[:, 0:128] * total[:, 0:128]
            for t in range(1, LW // 128):
                squares = squares + total[:, t * 128 : t * 128 + 128] * total[:, t * 128 : t * 128 + 128]
            square[v] = squares if q == 0 else square[v] + squares

    msg[...] = jnp.zeros_like(msg)
    for k in range(NB):
        multiply_first(k)
        build_first(k, 0)
        if k == 0:
            pl.semaphore_wait(barrier, 15)
            tell(0)
        send_first(k, 0)

    odd.wait()

    def spread_odd(i, carry):
        flat[...] = to_v[pl.ds(i * 256, 256)].astype(F32).reshape(2048, 128)
        h = i // 2
        w = pl.multiple_of((i % 2) * 128, 128)
        for lt in range(8):
            for s in range(2):
                within = (lt % 4) * 128
                lo = (within // LW) * 4 * LW + s * 2 * LW + (lt // 4) * LW + within % LW
                tb[h, core, pl.ds(w, 128), lo : lo + 128] = flat[pl.ds(lt * 2 + s, 128, stride=16), :].astype(BF16)
        return carry

    lax.fori_loop(0, 2, spread_odd, 0)
    reduce_first(0, 0)
    lax.fori_loop(2, 4, spread_odd, 0)
    for h in range(2):
        send(tb.at[h, core], tb.at[h, core], tb_ssem, tb_rsem, at(x, y, z, 1 - core))
    hear(0)
    tell(1)
    reduce_first(1, 0)
    reduce_first(2, 0)
    for k in range(NB):
        build_first(k, 1)
    hear(1)
    tell(2)
    for k in range(NB):
        finish_chosen(k)
    for k in range(NB):
        send_first(k, 1)
    hear(2)
    wait_bytes(tb.at[:, 0], tb_rsem)
    for k in range(NB):
        gather_left(k)
    for q in range(NQ):
        multiply_second(q)
        ring_step(q, 0)
    for s in range(1, HZ):
        for q in range(NQ):
            ring_step(q, s)
        if s == 2:
            for k in range(NB):
                reduce_first(k, 1)
        if s == 4:
            for k in range(NB):
                finish_other(k)
            n0r[z] = msg[0:1, :]
            nfs[0:1, :] = msg[0:1, :]

            @pl.when(z != row)
            def _():
                send(nfs.at[0:1], n0r.at[z], n0_ssem, n0_rsem, at(x, y, row, core))

    for q in range(NQ):
        ring_end(q)

    own = norms_to_lanes(square[0], GROUP, 0) + norms_to_lanes(square[1], GROUP, 32)
    nfs[1:2, :] = own

    @pl.when(z == row)
    def _():
        wait_bytes(n0r.at[0 : NZ - 1], n0_rsem)
        nfs[1:2, :] = own + jnp.sum(n0r[...], axis=0)

    nfr[row] = nfs[1:2, :]
    for dx in (2, 1, 3, 0):
        for dy in (2, 1, 3, 0):
            if dx or dy:
                send(nfs.at[1:2], nfr.at[row], nf_ssem, nf_rsem, at((x + dx) % NA, (y + dy) % NA, z, core))

    wait_bytes(r1.at[:, :, :, 0:7], s1_sem)
    wait_bytes(r2.at[:, :, 0:3], s2_sem)
    wait_bytes(r2o.at[:, :, 0:3], s2o_sem)
    wait_bytes(g_buf.at[:, :, 0:3], gb_ssem)
    wait_bytes(tb.at[:, 0], tb_ssem)
    wait_bytes(zr, z_ssem)

    @pl.when(z != row)
    def _():
        wait_bytes(n0r.at[0], n0_ssem)

    wait_bytes(nfr.at[0 : G - 1], nf_rsem)
    norms = jnp.sum(nfr[...], axis=0)
    both = norms + pltpu.roll(norms, 96, 1)
    chosen_ref[0:1, :] = pltpu.roll(norms, 64, 1)[:, :GROUP]
    chosen_ref[1:2, :] = norms[:, :GROUP]
    both_ref[0:1, :] = pltpu.roll(both, 64, 1)[:, :GROUP]
    both_ref[1:2, :] = both[:, :GROUP]
    column = jnp.sum(jnp.where(lane == sub, jnp.broadcast_to(norms, (GROUP, 128)), 0.0), axis=1, keepdims=True)
    out_ref[...] = fin[...] * jnp.sqrt(CHI / column)
    wait_bytes(nfr.at[0 : G - 1], nf_ssem)


def per_device(environment, even_site, odd_site, outcomes, basis_codes):
    samples, left = environment.shape
    env = environment.reshape(2 * G, NB, SB, left)
    te = even_site.reshape(left, 2, 4, 128).transpose(0, 2, 1, 3).reshape(left, 8, 128)
    to = odd_site.reshape(512, 2, 8, 128).transpose(0, 2, 1, 3).reshape(1024, 8, 128)
    vmem = pl.BlockSpec(memory_space=pltpu.VMEM)
    hbm = pl.BlockSpec(memory_space=pl.ANY)
    dma = pltpu.SemaphoreType.DMA
    nz_slots = 4 * HZ - 2
    final, chosen_norms, both_norms = pl.pallas_call(
        kernel,
        out_shape=(
            jax.ShapeDtypeStruct((GROUP, RIGHT), F32),
            jax.ShapeDtypeStruct((2, GROUP), F32),
            jax.ShapeDtypeStruct((2, GROUP), F32),
        ),
        in_specs=[hbm] * 5,
        out_specs=(vmem,) * 3,
        scratch_shapes=[
            pltpu.VMEM((2 * G, NB, SB, left), BF16),
            pltpu.VMEM((left, 8, 128), BF16),
            pltpu.VMEM((1024, 8, 128), BF16),
            pltpu.VMEM((2, samples), jnp.int32),
            pltpu.VMEM((2, samples), jnp.int32),
            pltpu.VMEM((2048, 128), F32),
            pltpu.VMEM((left, 2 * COLS), BF16),
            pltpu.VMEM((NB, 2 * G * SB, 2 * COLS), F32),
            pltpu.VMEM((2, samples, 128), F32),
            pltpu.VMEM((NB, 2, 2, 2, NA, NA, R, 128), BF16),
            pltpu.VMEM((NB, 2, 2, 2 * NA, NA, R, 128), BF16),
            pltpu.VMEM((NB, 2, 2, NA, 2, R, 128), BF16),
            pltpu.VMEM((NB, 2, NA, NA, 2, R, 128), BF16),
            pltpu.VMEM((NB, 2, NA, 2, R, 128), BF16),
            pltpu.VMEM((NB, 2, NA, NA, 2, R, 128), BF16),
            pltpu.VMEM((NB * G * SB, 1024), BF16),
            pltpu.VMEM((2, 2, 256, 2 * RIGHT), BF16),
            pltpu.VMEM((NQ, NB * G * SB, 4 * LW), F32),
            pltpu.VMEM((2, NQ, NZ, RZ, LW), BF16),
            pltpu.VMEM((NQ, nz_slots, RZ, LW), BF16),
            pltpu.VMEM((NQ, nz_slots, RZ, LW), BF16),
            pltpu.VMEM((GROUP, RIGHT), F32),
            pltpu.VMEM((2, RZ, 128), F32),
            pltpu.VMEM((8, 128), F32),
            pltpu.VMEM((NZ, 1, 128), F32),
            pltpu.VMEM((8, 128), F32),
            pltpu.VMEM((G, 1, 128), F32),
            dma((4,)),
            dma((4,)),
            dma,
            dma((NB, 2, 2)),
            dma,
            dma,
            dma((NB, 2, 2)),
            dma,
            dma((NB, 2)),
            dma,
            dma,
            dma,
            dma((NQ, nz_slots)),
            dma,
            dma,
            dma,
            dma,
            pltpu.SemaphoreType.REGULAR((3,)),
        ],
        compiler_params=pltpu.CompilerParams(
            collective_id=0, has_side_effects=True, vmem_limit_bytes=60 * 1024 * 1024
        ),
    )(env, te, to, outcomes, basis_codes)
    return final.astype(BF16), chosen_norms / both_norms


def solution(mesh):
    placed = (P(None, "row"), P("row", None, "col"), P("col", None, "row"), P(), P())
    return jax.shard_map(
        per_device,
        mesh=mesh,
        in_specs=placed,
        out_specs=(P("col", "row"), P(None, "col")),
        check_vma=False,
    )
```

```python
import jax
import jax.numpy as jnp
from jax import lax
from jax.experimental import pallas as pl
from jax.experimental.pallas import tpu as pltpu
from jax.sharding import PartitionSpec as P

CHI = 16384
HALF_ROOT = 0.7071067811865476
F32 = jnp.float32
BF16 = jnp.bfloat16
MESH = pl.DeviceIdType.MESH

NA = 4
NZ = 16
G = NA * NA
HZ = NZ // 2
GROUP = 24
NB = 3
SB = GROUP // NB
R = 2 * SB
COLS = 512
RIGHT = 1024
NQ = 4
LW = 512 // NQ
RZ = 2 * GROUP
AHEAD = True


def coefficients(sel):
    rotated = sel >= 1.5
    odd = (sel == 1.0) | (sel == 3.0)
    sign = jnp.where(odd, -HALF_ROOT, HALF_ROOT)
    a = jnp.where(rotated, HALF_ROOT, jnp.where(odd, 0.0, 1.0))
    b = jnp.where(rotated, sign, jnp.where(odd, 1.0, 0.0))
    c = jnp.where(rotated, HALF_ROOT, jnp.where(odd, 1.0, 0.0))
    d = jnp.where(rotated, -sign, jnp.where(odd, 0.0, 1.0))
    return ((a, b), (c, d))


def kernel(
    env_hbm,
    te_hbm,
    to_hbm,
    outcomes_hbm,
    basis_hbm,
    out_ref,
    chosen_ref,
    both_ref,
    env_v,
    te_v,
    to_v,
    outcomes,
    basis,
    flat,
    w0,
    acc0,
    sel,
    s1,
    r1,
    s2,
    r2,
    r2o,
    g_buf,
    lhs,
    tb,
    acc1,
    part,
    zs,
    zr,
    cf,
    mine,
    fin,
    square,
    msg,
    n0r,
    nfs,
    nfr,
    load_sem,
    te_sem,
    s1_sem,
    r1_sem,
    s2_sem,
    s2o_sem,
    r2_sem,
    gb_ssem,
    gb_rsem,
    tb_ssem,
    tb_rsem,
    z_ssem,
    z_rsem,
    m_ssem,
    m_rsem,
    n0_ssem,
    n0_rsem,
    nf_ssem,
    nf_rsem,
    known,
):
    row = lax.axis_index("row")
    col = lax.axis_index("col")
    z = col // 2
    core = col % 2
    x = row % NA
    y = row // NA
    par = (core + z) % 2
    first_place = (x, y)
    second_place = (y, x)

    def at(px, py, pz, pc):
        return {"row": py * NA + px, "col": pz * 2 + pc}

    def peer(f, a, b, pc):
        return at(a, b, z, pc) if f == 0 else at(b, a, z, pc)

    def send(src, dst, ssem, rsem, device):
        pltpu.make_async_remote_copy(
            src_ref=src, dst_ref=dst, send_sem=ssem, recv_sem=rsem, device_id=device, device_id_type=MESH
        ).start()

    def wait_bytes(ref, sem):
        pltpu.make_async_copy(ref, ref, sem).wait()

    codes = [
        pltpu.make_async_copy(outcomes_hbm, outcomes, load_sem.at[0]),
        pltpu.make_async_copy(basis_hbm, basis, load_sem.at[1]),
    ]
    even = [
        pltpu.make_async_copy(te_hbm.at[pl.ds(i * 256, 256)], te_v.at[pl.ds(i * 256, 256)], te_sem.at[i])
        for i in range(4)
    ]
    vectors = pltpu.make_async_copy(env_hbm, env_v, load_sem.at[2])
    odd = pltpu.make_async_copy(to_hbm, to_v, load_sem.at[3])
    for load in (*codes, *even, vectors):
        load.start()

    barrier = pltpu.get_barrier_semaphore()

    def signal(sem, device):
        pl.semaphore_signal(sem, inc=1, device_id=device, device_id_type=MESH)

    for dc in range(2):
        if dc:
            signal(barrier, at(x, y, z, 1 - core))
        for d in range(1, NA):
            signal(barrier, at((x + d) % NA, y, z, (core + dc) % 2))
            signal(barrier, at(x, (y + d) % NA, z, (core + dc) % 2))
        for dz in (1, NZ - 1):
            signal(barrier, at(x, y, (z + dz) % NZ, (core + dc) % 2))

    def tell(i):
        for dz in (2**i, NZ - 2**i):
            for dc in range(2):
                signal(known.at[i], at(x, y, (z + dz) % NZ, (core + dc) % 2))

    def hear(i):
        pl.semaphore_wait(known.at[i], 4)

    for load in codes:
        load.wait()
    eye = lax.broadcasted_iota(jnp.int32, (128, 128), 0) == lax.broadcasted_iota(jnp.int32, (128, 128), 1)
    for s in range(2):
        for j in range(6):
            lanes = slice(j * 128, (j + 1) * 128)
            code = (2 * basis[s : s + 1, lanes] + outcomes[s : s + 1, lanes]).astype(F32)
            column = jnp.sum(jnp.where(eye, jnp.broadcast_to(code, (128, 128)), 0.0), axis=1, keepdims=True)
            sel[s, j * 128 : (j + 1) * 128, :] = jnp.broadcast_to(column, (128, 128))

    for i in range(4):
        even[i].wait()
        for j in range(2):
            l0 = i * 256 + j * 128
            flat[j * 1024 : j * 1024 + 1024, :] = te_v[l0 : l0 + 128].astype(F32).reshape(1024, 128)
            for lt in range(4):
                for s in range(2):
                    lo = s * COLS + lt * 128
                    w0[l0 : l0 + 128, lo : lo + 128] = flat[
                        pl.ds(j * 1024 + lt * 2 + s, 128, stride=8), :
                    ].astype(BF16)
    odd.start()

    vectors.wait()

    def multiply_first(k):
        rows = env_v[:, k].reshape(2 * G * SB, 1024)
        for n in range(2):
            acc0[k, :, n * 512 : n * 512 + 512] = jnp.dot(
                rows, w0[:, n * 512 : n * 512 + 512], preferred_element_type=F32
            )

    def build_first(k, v):
        for gp in range(2 * G):
            g, p = gp // 2, gp % 2
            gx, gy = g % NA, g // NA
            rows = slice(gp * SB, gp * SB + SB)
            cu, cd = coefficients(sel[0, gp * GROUP + k * SB : gp * GROUP + k * SB + SB, :])[v]
            for f in range(2):
                halves = []
                for h in range(2):
                    lo = h * 256 + f * 128
                    halves.append(
                        cu * acc0[k, rows, lo : lo + 128] + cd * acc0[k, rows, COLS + lo : COLS + lo + 128]
                    )
                ga, gb = (gx, gy) if f == 0 else (gy, gx)
                s1[k, v, f, p, ga, gb] = jnp.concatenate(halves, axis=0).astype(BF16)

    def send_first(k, v):
        for da in (2, 1, 3, 0):
            for f in range(2):
                a = (first_place[f] + da) % NA
                for dc in range(2):
                    if da == 0 and dc == 0:
                        continue
                    pc = (core + dc) % 2
                    send(
                        s1.at[k, v, f, (pc + z) % 2, a],
                        r1.at[k, v, f, first_place[f] * 2 + core],
                        s1_sem,
                        r1_sem.at[k, v, f],
                        peer(f, a, second_place[f], pc),
                    )

    def reduce_first(k, v):
        for f in range(2):
            r1[k, v, f, first_place[f] * 2 + core] = s1[k, v, f, par, first_place[f]]
            wait_bytes(r1.at[k, v, f, 0:7], r1_sem.at[k, v, f])
            for b in range(NA):
                for c in range(2):
                    total = r1[k, v, f, c, b].astype(F32)
                    for a in range(1, NA):
                        total = total + r1[k, v, f, a * 2 + c, b].astype(F32)
                    s2[k, v, f, b, c] = total.astype(BF16)
            for db in (2, 1, 3):
                b = (second_place[f] + db) % NA
                device = peer(f, first_place[f], b, core)
                if v == 0:
                    send(s2.at[k, v, f], r2.at[k, f, second_place[f]], s2_sem, r2_sem.at[k, v, f], device)
                else:
                    send(s2.at[k, v, f, b], r2o.at[k, f, second_place[f]], s2o_sem, r2_sem.at[k, v, f], device)

    lane = lax.broadcasted_iota(jnp.int32, (GROUP, 128), 1)
    sub = lax.broadcasted_iota(jnp.int32, (GROUP, 128), 0)

    def norms_to_lanes(squares, count, base):
        sums = jnp.sum(squares, axis=1, keepdims=True)
        column = sums[:count] + sums[count:]
        return jnp.sum(jnp.where(lane[:count] == sub[:count] + base, column, 0.0), axis=0, keepdims=True)

    def finish_chosen(k):
        squares = jnp.zeros((R, 128), F32)
        for f in range(2):
            r2[k, f, second_place[f]] = s2[k, 0, f]
            wait_bytes(r2.at[k, f, 0:3], r2_sem.at[k, 0, f])
            for b in range(NA):
                for c in range(2):
                    total = r2[k, f, 0, b, c].astype(F32)
                    for e in range(1, NA):
                        total = total + r2[k, f, e, b, c].astype(F32)
                    g_buf[k, f, first_place[f], b, c] = total.astype(BF16)
            for da in (2, 1, 3):
                a = (first_place[f] + da) % NA
                here = g_buf.at[k, f, first_place[f]]
                send(here, here, gb_ssem, gb_rsem.at[k, f], peer(f, a, second_place[f], core))
        for f in range(2):
            for c in range(2):
                total = r2[k, f, 0, second_place[f], c].astype(F32)
                for e in range(1, NA):
                    total = total + r2[k, f, e, second_place[f], c].astype(F32)
                squares = squares + total * total
        msg[0:1, :] += norms_to_lanes(squares, SB, 64 + k * SB)

    def finish_other(k):
        squares = jnp.zeros((R, 128), F32)
        for f in range(2):
            r2o[k, f, second_place[f]] = s2[k, 1, f, second_place[f]]
            wait_bytes(r2o.at[k, f, 0:3], r2_sem.at[k, 1, f])
            for c in range(2):
                total = r2o[k, f, 0, c].astype(F32)
                for e in range(1, NA):
                    total = total + r2o[k, f, e, c].astype(F32)
                squares = squares + total * total
        msg[0:1, :] += norms_to_lanes(squares, SB, 96 + k * SB)

    def gather_left(k):
        for f in range(2):
            wait_bytes(g_buf.at[k, f, 0:3], gb_rsem.at[k, f])

        def pair(j, carry):
            m0 = pl.multiple_of(k * G * SB + j * 2 * SB, 2 * SB)
            gy = j // 2
            for f in range(2):
                for c in range(2):
                    two = []
                    for e in range(2):
                        gx = (2 * j + e) % NA
                        ga, gb = (gx, gy) if f == 0 else (gy, gx)
                        two.append(g_buf[k, f, ga, gb, c].astype(F32))
                    for h in range(2):
                        lo = h * 512 + c * 256 + f * 128
                        lhs[pl.ds(m0, 2 * SB), lo : lo + 128] = jnp.concatenate(
                            [t[h * SB : (h + 1) * SB] for t in two], axis=0
                        ).astype(BF16)
            return carry

        lax.fori_loop(0, G // 2, pair, 0, unroll=2)

    def second_coefficients():
        for k in range(NB):
            for g in range(G):
                samples = pl.ds(pl.multiple_of((2 * g + par) * GROUP + k * SB, 8), SB)
                pairs = coefficients(sel[1, samples, :])
                for v in range(2):
                    for e in range(2):
                        cf[v, e, (k * G + g) * SB : (k * G + g) * SB + SB, :] = pairs[v][e]

    def multiply_second(q):
        for n in range(4 * LW // 256):
            lo = q * 4 * LW + n * 256
            acc1[q, :, n * 256 : n * 256 + 256] = jnp.dot(
                lhs[...], tb[:, :, :, lo : lo + 256].reshape(1024, 256), preferred_element_type=F32
            )

    def build_second(q):
        for g in range(G):
            for t in range(LW // 128):
                chunks = ([], [])
                for h in range(2):
                    for k in range(NB):
                        rows = slice((k * G + g) * SB, (k * G + g) * SB + SB)
                        lo = h * LW + t * 128
                        up = acc1[q, rows, lo : lo + 128]
                        down = acc1[q, rows, 2 * LW + lo : 2 * LW + lo + 128]
                        for v in range(2):
                            chunks[v].append(cf[v, 0, rows, :] * up + cf[v, 1, rows, :] * down)
                for v in range(2):
                    part[v, q, g, :, t * 128 : t * 128 + 128] = jnp.concatenate(chunks[v], axis=0).astype(BF16)

    def own_part(q):
        @pl.when(z % 2 == 0)
        def _():
            mine[:, q] = part[:, q, z]

        @pl.when(z % 2 == 1)
        def _():
            for v in range(2):
                send(part.at[v, q, z], mine.at[v, q], m_ssem, m_rsem.at[q], at(x, y, z, 1 - core))

    def hops(v, d):
        return HZ - v if d == 0 else HZ - 1 + v

    def slot(v, d, s):
        return {(0, 0): 0, (0, 1): HZ, (1, 0): 2 * HZ - 1, (1, 1): 3 * HZ - 2}[v, d] + s

    def ring_step(q, s):
        for v in range(2):
            for d in range(2):
                n = hops(v, d)
                if s >= n:
                    continue
                owner = (z + n - s) % NZ if d == 0 else (z + NZ - n + s) % NZ
                step = 1 if d == 0 else NZ - 1
                here = slot(v, d, s)
                if s == 0:
                    src = part.at[v, q, owner]
                else:
                    wait_bytes(zr.at[q, here - 1], z_rsem.at[q, here - 1])
                    zs[q, here] = (zr[q, here - 1].astype(F32) + part[v, q, owner].astype(F32)).astype(BF16)
                    src = zs.at[q, here]
                target = par if s == n - 1 else 1 - core
                send(src, zr.at[q, here], z_ssem, z_rsem.at[q, here], at(x, y, (z + step) % NZ, target))

    def ring_end(q):
        @pl.when(z % 2 == 1)
        def _():
            wait_bytes(mine.at[:, q], m_rsem.at[q])

        for v in range(2):
            total = mine[v, q].astype(F32)
            for d in range(2):
                last = slot(v, d, hops(v, d) - 1)
                wait_bytes(zr.at[q, last], z_rsem.at[q, last])
                total = total + zr[q, last].astype(F32)
            if v == 0:
                for h in range(2):
                    fin[:, h * 512 + q * LW : h * 512 + q * LW + LW] = total[h * GROUP : (h + 1) * GROUP]
            squares = total[:, 0:128] * total[:, 0:128]
            for t in range(1, LW // 128):
                squares = squares + total[:, t * 128 : t * 128 + 128] * total[:, t * 128 : t * 128 + 128]
            square[v] = squares if q == 0 else square[v] + squares

    given_here = (z == row) & (par == core)
    msg[...] = jnp.zeros_like(msg)
    for k in range(NB):
        multiply_first(k)
        build_first(k, 0)
        if k == 0:
            pl.semaphore_wait(barrier, 17)
            tell(0)
        send_first(k, 0)

    odd.wait()

    def spread_odd(i, carry):
        flat[...] = to_v[pl.ds(i * 256, 256)].astype(F32).reshape(2048, 128)
        h = i // 2
        w = pl.multiple_of((i % 2) * 128, 128)
        for lt in range(8):
            for s in range(2):
                within = (lt % 4) * 128
                lo = (within // LW) * 4 * LW + s * 2 * LW + (lt // 4) * LW + within % LW
                tb[h, core, pl.ds(w, 128), lo : lo + 128] = flat[pl.ds(lt * 2 + s, 128, stride=16), :].astype(BF16)
        return carry

    lax.fori_loop(0, 2, spread_odd, 0)
    reduce_first(0, 0)
    lax.fori_loop(2, 4, spread_odd, 0)
    for h in range(2):
        send(tb.at[h, core], tb.at[h, core], tb_ssem, tb_rsem, at(x, y, z, 1 - core))
    reduce_first(1, 0)
    hear(0)
    tell(1)
    reduce_first(2, 0)
    finish_chosen(0)
    build_first(0, 1)
    build_first(1, 1)
    finish_chosen(1)
    hear(1)
    tell(2)
    build_first(2, 1)
    finish_chosen(2)
    for k in range(NB):
        send_first(k, 1)
    second_coefficients()
    hear(2)
    wait_bytes(tb.at[:, 0], tb_rsem)
    for k in range(NB):
        gather_left(k)
    multiply_second(0)
    for q in range(NQ):
        if AHEAD and q + 1 < NQ:
            multiply_second(q + 1)
        build_second(q)
        ring_step(q, 0)
        if not AHEAD and q + 1 < NQ:
            multiply_second(q + 1)
    for s in range(1, HZ):
        for q in range(NQ):
            if s == 1:
                own_part(q)
            ring_step(q, s)
        if s == 2:
            for k in range(NB):
                reduce_first(k, 1)
        if s == 4:
            for k in range(NB):
                finish_other(k)
            nfs[0:1, :] = msg[0:1, :]

            @pl.when(given_here)
            def _():
                n0r[z] = msg[0:1, :]

            @pl.when(jnp.logical_not(given_here))
            def _():
                send(nfs.at[0:1], n0r.at[z], n0_ssem, n0_rsem, at(x, y, row, par))

    for q in range(NQ):
        ring_end(q)

    own = norms_to_lanes(square[0], GROUP, 0) + norms_to_lanes(square[1], GROUP, 32)
    nfs[1:2, :] = own

    @pl.when(given_here)
    def _():
        wait_bytes(n0r.at[0 : NZ - 1], n0_rsem)

    @pl.when((z == row) & (par != core))
    def _():
        wait_bytes(n0r, n0_rsem)

    @pl.when(z == row)
    def _():
        nfs[1:2, :] = own + jnp.sum(n0r[...], axis=0)

    nfr[row] = nfs[1:2, :]
    for dx in (2, 1, 3, 0):
        for dy in (2, 1, 3, 0):
            if dx or dy:
                send(nfs.at[1:2], nfr.at[row], nf_ssem, nf_rsem, at((x + dx) % NA, (y + dy) % NA, z, core))

    wait_bytes(r1.at[:, :, :, 0:7], s1_sem)
    wait_bytes(r2.at[:, :, 0:3], s2_sem)
    wait_bytes(r2o.at[:, :, 0:3], s2o_sem)
    wait_bytes(g_buf.at[:, :, 0:3], gb_ssem)
    wait_bytes(tb.at[:, 0], tb_ssem)
    wait_bytes(zr, z_ssem)

    @pl.when(jnp.logical_not(given_here))
    def _():
        wait_bytes(n0r.at[0], n0_ssem)

    @pl.when(z % 2 == 1)
    def _():
        wait_bytes(mine, m_ssem)

    wait_bytes(nfr.at[0 : G - 1], nf_rsem)
    norms = jnp.sum(nfr[...], axis=0)
    both = norms + pltpu.roll(norms, 96, 1)
    chosen_ref[0:1, :] = pltpu.roll(norms, 64, 1)[:, :GROUP]
    chosen_ref[1:2, :] = norms[:, :GROUP]
    both_ref[0:1, :] = pltpu.roll(both, 64, 1)[:, :GROUP]
    both_ref[1:2, :] = both[:, :GROUP]
    column = jnp.sum(jnp.where(lane == sub, jnp.broadcast_to(norms, (GROUP, 128)), 0.0), axis=1, keepdims=True)
    out_ref[...] = fin[...] * jnp.sqrt(CHI / column)
    wait_bytes(nfr.at[0 : G - 1], nf_ssem)


def per_device(environment, even_site, odd_site, outcomes, basis_codes):
    samples, left = environment.shape
    env = environment.reshape(2 * G, NB, SB, left)
    te = even_site.reshape(left, 2, 4, 128).transpose(0, 2, 1, 3).reshape(left, 8, 128)
    to = odd_site.reshape(512, 2, 8, 128).transpose(0, 2, 1, 3).reshape(1024, 8, 128)
    vmem = pl.BlockSpec(memory_space=pltpu.VMEM)
    hbm = pl.BlockSpec(memory_space=pl.ANY)
    dma = pltpu.SemaphoreType.DMA
    nz_slots = 4 * HZ - 2
    final, chosen_norms, both_norms = pl.pallas_call(
        kernel,
        out_shape=(
            pltpu.VMEM((GROUP, RIGHT), F32),
            pltpu.VMEM((2, GROUP), F32),
            pltpu.VMEM((2, GROUP), F32),
        ),
        in_specs=[hbm] * 5,
        out_specs=(vmem,) * 3,
        scratch_shapes=[
            pltpu.VMEM((2 * G, NB, SB, left), BF16),
            pltpu.VMEM((left, 8, 128), BF16),
            pltpu.VMEM((1024, 8, 128), BF16),
            pltpu.VMEM((2, samples), jnp.int32),
            pltpu.VMEM((2, samples), jnp.int32),
            pltpu.VMEM((2048, 128), F32),
            pltpu.VMEM((left, 2 * COLS), BF16),
            pltpu.VMEM((NB, 2 * G * SB, 2 * COLS), F32),
            pltpu.VMEM((2, samples, 128), F32),
            pltpu.VMEM((NB, 2, 2, 2, NA, NA, R, 128), BF16),
            pltpu.VMEM((NB, 2, 2, 2 * NA, NA, R, 128), BF16),
            pltpu.VMEM((NB, 2, 2, NA, 2, R, 128), BF16),
            pltpu.VMEM((NB, 2, NA, NA, 2, R, 128), BF16),
            pltpu.VMEM((NB, 2, NA, 2, R, 128), BF16),
            pltpu.VMEM((NB, 2, NA, NA, 2, R, 128), BF16),
            pltpu.VMEM((NB * G * SB, 1024), BF16),
            pltpu.VMEM((2, 2, 256, 2 * RIGHT), BF16),
            pltpu.VMEM((NQ, NB * G * SB, 4 * LW), F32),
            pltpu.VMEM((2, NQ, NZ, RZ, LW), BF16),
            pltpu.VMEM((NQ, nz_slots, RZ, LW), BF16),
            pltpu.VMEM((NQ, nz_slots, RZ, LW), BF16),
            pltpu.VMEM((2, 2, NB * G * SB, 128), F32),
            pltpu.VMEM((2, NQ, RZ, LW), BF16),
            pltpu.VMEM((GROUP, RIGHT), F32),
            pltpu.VMEM((2, RZ, 128), F32),
            pltpu.VMEM((8, 128), F32),
            pltpu.VMEM((NZ, 1, 128), F32),
            pltpu.VMEM((8, 128), F32),
            pltpu.VMEM((G, 1, 128), F32),
            dma((4,)),
            dma((4,)),
            dma,
            dma((NB, 2, 2)),
            dma,
            dma,
            dma((NB, 2, 2)),
            dma,
            dma((NB, 2)),
            dma,
            dma,
            dma,
            dma((NQ, nz_slots)),
            dma,
            dma((NQ,)),
            dma,
            dma,
            dma,
            dma,
            pltpu.SemaphoreType.REGULAR((3,)),
        ],
        compiler_params=pltpu.CompilerParams(
            collective_id=0, has_side_effects=True, vmem_limit_bytes=60 * 1024 * 1024
        ),
    )(env, te, to, outcomes, basis_codes)
    return final.astype(BF16), chosen_norms / both_norms


def solution(mesh):
    placed = (P(None, "row"), P("row", None, "col"), P("col", None, "row"), P(), P())
    return jax.shard_map(
        per_device,
        mesh=mesh,
        in_specs=placed,
        out_specs=(P("col", "row"), P(None, "col")),
        check_vma=False,
    )
```
